256 devices in a mesh: lat: 8 (over x, core), lon: 32 (over z, y).
Axes of the slice: x: 4, y: 4, z: 8, core: 2. Of those that a mesh axis runs over, the one named last changes fastest.
Arguments:
- grid: bfloat16 [720, 1440, 384], P('lat', 'lon'), may hold values from -33 to 33
- legendre: bfloat16 [384, 720, 384], P('lon', 'lat'), may hold values from -0.021606041 to 0.021606041, as said below
Outputs:
- normalized: bfloat16 [384, 384, 2, 384], P('lat', 'lon')
- spread: float32 [384], P('lat')
The draws below stay inside these ranges and needn't reach their ends.
Inputs may be any that keep to these rules, and one draw needn't show every extreme that they name: legendre[m, j, l] is zero wherever l < m.
All inputs are finite; a program needn't handle non-finite values.
Results may differ from the reference program's by a relative error of at most 0.014.
Values may be sent and summed in bfloat16 or wider, within the bound.
A program may use at most 64 MiB of HBM per device.

```python
import math
import jax
import jax.numpy as jnp
from jax import lax

NLAT = 720
NLON = 1440
DEG = 384
CHANNELS = 64
MEMBERS = 6
FIELDS = 384
N_LAT = 8


def draw_grid(key, part):
    scale_key = jax.random.fold_in(key, 11)
    member_key = jax.random.fold_in(key, 12)
    channel_scale = jnp.exp(jax.random.uniform(scale_key, (CHANNELS,), jnp.float32, math.log(0.3), math.log(3.0)))
    values = jnp.clip(jax.random.normal(member_key, (NLAT, NLON, MEMBERS, CHANNELS), jnp.float32), -6.0, 6.0)
    values = values * channel_scale
    return values.reshape(NLAT, NLON, MEMBERS * CHANNELS).astype(jnp.bfloat16)


def draw_legendre(key, part):
    wobble_key = jax.random.fold_in(key, 21)
    entry_key = jax.random.fold_in(key, 22)
    order_ids = jnp.arange(DEG, dtype=jnp.int32)
    ramp = jnp.sqrt(1.0 + 2.0 * order_ids.astype(jnp.float32) / DEG)
    wobble = jnp.exp(jax.random.uniform(wobble_key, (DEG,), jnp.float32, math.log(0.5), math.log(2.0)))
    entries = jnp.clip(jax.random.normal(entry_key, (DEG, NLAT, DEG), jnp.float32), -6.0, 6.0)
    triangle = (order_ids[None, None, :] >= order_ids[:, None, None]).astype(jnp.float32)
    factor = (ramp * wobble)[:, None, None] * (1.0 / math.sqrt(NLAT * NLON))
    return (entries * factor * triangle).astype(jnp.bfloat16)


def setup_inputs(seed: int = 0) -> dict:
    arg_keys = jax.random.split(jax.random.key(seed), 3)
    grid = draw_grid(jax.random.fold_in(arg_keys[2], 71), 0)
    legendre = draw_legendre(jax.random.fold_in(arg_keys[2], 71), 0)
    return dict(grid=grid, legendre=legendre)


epsilon = 1e-06

def spectral_table():
    longitude = jnp.arange(NLON, dtype=jnp.int32)[:, None]
    order_ids = jnp.arange(DEG, dtype=jnp.int32)[None, :]
    phase = longitude * order_ids % NLON
    angle = phase.astype(jnp.float32) * (2.0 * math.pi / NLON)
    stacked = jnp.stack([jnp.cos(angle), -jnp.sin(angle)], axis=1)
    return stacked.astype(jnp.bfloat16)

def reference(grid, legendre):
    lat_rows = NLAT // N_LAT
    order_rows = DEG // 4
    basis = lax.optimization_barrier(spectral_table()).astype(jnp.float32)

    def order_block(block_id):
        first_order = (block_id * order_rows).astype(jnp.int32)
        basis_part = lax.dynamic_slice_in_dim(basis, first_order, order_rows, 2)

        def band_step(band_id, running):
            first_cycle = (band_id * lat_rows).astype(jnp.int32)
            lat_block = lax.dynamic_slice_in_dim(grid, first_cycle, lat_rows, 0).astype(jnp.float32)
            spectrum = jnp.einsum('jkf,krm->jfrm', lat_block, basis_part)
            spectrum = lax.optimization_barrier(spectrum.astype(jnp.bfloat16)).astype(jnp.float32)
            weights = lax.dynamic_slice(legendre, (first_order, first_cycle, jnp.zeros((), jnp.int32)), (order_rows, lat_rows, DEG)).astype(jnp.float32)
            band_part = jnp.einsum('jfrm,mjl->lmrf', spectrum, weights)
            band_part = lax.optimization_barrier(band_part.astype(jnp.bfloat16)).astype(jnp.float32)
            return running + band_part
        start_sum = jnp.zeros((DEG, order_rows, 2, FIELDS), jnp.float32)
        return lax.fori_loop(0, N_LAT, band_step, start_sum)
    stacked = lax.map(order_block, jnp.arange(4, dtype=jnp.int32))
    coeffs = jnp.transpose(stacked, (1, 0, 2, 3, 4)).reshape(DEG, DEG, 2, FIELDS)
    by_member = coeffs.reshape(DEG, DEG, 2, MEMBERS, CHANNELS)
    deviation = by_member - lax.optimization_barrier(jnp.mean(by_member, axis=3, keepdims=True))
    degree = jnp.arange(DEG, dtype=jnp.int32).astype(jnp.float32)
    divisor = (MEMBERS - 1) * CHANNELS * (2.0 * degree + 1.0)
    spread = lax.optimization_barrier(jnp.sum(deviation * deviation, axis=(1, 2, 3, 4))) / divisor
    normalized = coeffs * lax.rsqrt(spread + epsilon)[:, None, None, None]
    return (normalized.astype(jnp.bfloat16), spread)
```

```python
import math

import jax
import jax.numpy as jnp
import numpy as np
from jax import lax
from jax.experimental import pallas as pl
from jax.experimental.pallas import tpu as pltpu
from jax.sharding import PartitionSpec as P

NLON = 1440
DEG = 384
CHANNELS = 64
MEMBERS = 6
FIELDS = 384
LAT = 8
LON = 32
ROWS = 90
LON_ROWS = 45
PADDED = 48
ORDERS = 12
DEGREES = 48
UNITS = 3
CHUNKS = 3
JPAD = 96
EPSILON = 1e-06
MESH = pl.DeviceIdType.MESH


def spectral_table():
    k = np.arange(NLON, dtype=np.int64)[:, None]
    m = np.arange(DEG, dtype=np.int64)[None, :]
    angle = ((k * m) % NLON).astype(np.float32) * np.float32(2.0 * math.pi / NLON)
    table = np.stack([np.cos(angle), -np.sin(angle)], axis=2).astype(np.float32)
    table = table.reshape(LON, LON_ROWS, LON, LAT, UNITS)
    padded = np.zeros((LON, PADDED, LON, LAT, UNITS), np.float32)
    padded[:, :LON_ROWS] = table
    return padded.transpose(3, 2, 4, 0, 1).reshape(2 * DEG, LON * PADDED).astype(jnp.bfloat16)


def wait_bytes(ref, sem):
    pltpu.make_async_copy(ref, ref, sem).wait()


def swap_matrix(major, minor):
    size = major * minor
    out_row = lax.broadcasted_iota(jnp.int32, (size, size), 0)
    in_row = lax.broadcasted_iota(jnp.int32, (size, size), 1)
    wanted = (out_row % major) * minor + out_row // major
    return (in_row == wanted).astype(jnp.float32).astype(jnp.bfloat16)


def kernel(
    grid_ref,
    leg_ref,
    basis_ref,
    out_ref,
    spread_ref,
    recv,
    basis,
    spec,
    mixed,
    sent,
    spectral,
    leg_raw,
    leg,
    part,
    coeffs,
    squares,
    all_squares,
    swap_spec,
    swap_leg,
    swap_out,
    basis_sem,
    grid_send,
    grid_recv,
    leg_send,
    leg_recv,
    mix_send,
    mix_recv,
    spec_send,
    spec_recv,
    coef_send,
    coef_recv,
    sq_send,
    sq_recv,
):
    b = lax.axis_index("lat")
    g = lax.axis_index("lon")

    def lon_peer(i):
        return (g + i) % LON

    def lat_peer(i):
        return (b + i) % LAT

    def has_row(chunk, d):
        return (chunk < 2) | (d % 5 != 4)

    def row_of(chunk, d):
        return chunk * LON + d - jnp.where(chunk == 2, d // 5, 0)

    basis_copy = pltpu.make_async_copy(basis_ref, basis, basis_sem)
    basis_copy.start()
    barrier = pltpu.get_barrier_semaphore()

    @pl.loop(1, LON)
    def _(i):
        pl.semaphore_signal(barrier, inc=1, device_id={"lon": lon_peer(i)}, device_id_type=MESH)

    @pl.loop(1, LAT)
    def _(i):
        pl.semaphore_signal(barrier, inc=1, device_id={"lat": lat_peer(i)}, device_id_type=MESH)

    pl.semaphore_wait(barrier, LON + LAT - 2)

    @pl.loop(1, LAT)
    def _(i):
        u = lat_peer(i)
        pltpu.make_async_remote_copy(
            src_ref=leg_ref.at[pl.ds(UNITS * u // 2, 2)],
            dst_ref=leg_raw.at[b],
            send_sem=leg_send,
            recv_sem=leg_recv,
            device_id={"lat": u},
            device_id_type=MESH,
        ).start()

    pltpu.make_async_copy(leg_ref.at[pl.ds(UNITS * b // 2, 2)], leg_raw.at[b], leg_recv).start()

    @pl.loop(0, CHUNKS)
    def _(chunk):
        @pl.loop(1, LON)
        def _(i):
            d = lon_peer(i)

            @pl.when(has_row(chunk, d))
            def _():
                pltpu.make_async_remote_copy(
                    src_ref=grid_ref.at[row_of(chunk, d)],
                    dst_ref=recv.at[chunk, g],
                    send_sem=grid_send.at[chunk],
                    recv_sem=grid_recv.at[chunk],
                    device_id={"lon": d},
                    device_id_type=MESH,
                ).start()

        @pl.when(has_row(chunk, g))
        def _():
            pltpu.make_async_copy(grid_ref.at[row_of(chunk, g)], recv.at[chunk, g], grid_recv.at[chunk]).start()

    swap_spec[...] = swap_matrix(LAT, 32)
    swap_leg[...] = swap_matrix(LAT, 16)
    swap_out[...] = swap_matrix(2 * ORDERS, 16)
    spectral[:, ROWS:] = jnp.zeros((UNITS, JPAD - ROWS, LAT, FIELDS), spectral.dtype)

    wait_bytes(leg_raw, leg_recv)
    for which in range(2):
        for block in range(JPAD // 16):
            first = 16 * block
            rows = min(16, ROWS - first)
            piece = leg_raw[:, which, first : first + rows, :].astype(jnp.float32)
            if rows < 16:
                piece = jnp.concatenate([piece, jnp.zeros((LAT, 16 - rows, DEG), jnp.float32)], axis=1)
            piece = piece.reshape(LAT * 16, DEG).astype(jnp.bfloat16)
            moved = jnp.dot(swap_leg[...], piece, preferred_element_type=jnp.float32)
            leg[which, :, 128 * block : 128 * (block + 1)] = moved.T.astype(jnp.bfloat16)

    basis_copy.wait()

    @pl.loop(0, CHUNKS)
    def _(chunk):
        @pl.when(has_row(chunk, g))
        def _():
            wait_bytes(recv.at[chunk], grid_recv.at[chunk])
            values = recv[chunk].reshape(LON * PADDED, FIELDS)
            rows = jnp.dot(basis[...], values, preferred_element_type=jnp.float32)
            spec[chunk] = rows.astype(jnp.bfloat16).reshape(LAT, LON * UNITS, FIELDS)

            @pl.loop(1, LAT)
            def _(i):
                u = lat_peer(i)
                pltpu.make_async_remote_copy(
                    src_ref=spec.at[chunk, u],
                    dst_ref=mixed.at[chunk, b],
                    send_sem=mix_send.at[chunk],
                    recv_sem=mix_recv.at[chunk],
                    device_id={"lat": u},
                    device_id_type=MESH,
                ).start()

            pltpu.make_async_copy(spec.at[chunk, b], mixed.at[chunk, b], mix_recv.at[chunk]).start()
            wait_bytes(mixed.at[chunk], mix_recv.at[chunk])
            for block in range(3):
                piece = mixed[chunk, :, 32 * block : 32 * (block + 1), :].reshape(LAT * 32, FIELDS)
                moved = jnp.dot(swap_spec[...], piece, preferred_element_type=jnp.float32)
                sent[chunk, 32 * block : 32 * (block + 1)] = moved.reshape(32, LAT, FIELDS).astype(jnp.bfloat16)
            row = row_of(chunk, g)

            @pl.loop(1, LON)
            def _(i):
                d = lon_peer(i)
                pltpu.make_async_remote_copy(
                    src_ref=sent.at[chunk, pl.ds(UNITS * d, UNITS)],
                    dst_ref=spectral.at[:, row],
                    send_sem=spec_send.at[chunk],
                    recv_sem=spec_recv,
                    device_id={"lon": d},
                    device_id_type=MESH,
                ).start()

            pltpu.make_async_copy(sent.at[chunk, pl.ds(UNITS * g, UNITS)], spectral.at[:, row], spec_recv).start()

    wait_bytes(spectral.at[:, pl.ds(0, ROWS)], spec_recv)
    for unit in range(UNITS):
        which = (UNITS * b + unit) // 2 - UNITS * b // 2
        values = spectral[unit].astype(jnp.float32).reshape(JPAD * LAT, FIELDS).astype(jnp.bfloat16)
        total = jnp.dot(leg[which], values, preferred_element_type=jnp.float32)
        part[:, unit] = total.astype(jnp.bfloat16).reshape(LAT, DEGREES, FIELDS)

    @pl.loop(1, LAT)
    def _(i):
        u = lat_peer(i)
        pltpu.make_async_remote_copy(
            src_ref=part.at[u],
            dst_ref=coeffs.at[b],
            send_sem=coef_send,
            recv_sem=coef_recv,
            device_id={"lat": u},
            device_id_type=MESH,
        ).start()

    pltpu.make_async_copy(part.at[b], coeffs.at[b], coef_recv).start()
    wait_bytes(coeffs, coef_recv)

    acc = jnp.zeros((128, 128), jnp.float32)
    total = jnp.zeros((DEGREES, 128), jnp.float32)
    for u in range(LAT):
        for unit in range(UNITS):
            x = coeffs[u, unit].astype(jnp.float32)
            tiles = [x[:, 128 * t : 128 * (t + 1)] for t in range(3)]
            both = tiles[0] + tiles[1] + tiles[2]
            mean = (both + pltpu.roll(both, CHANNELS, 1)) * (1.0 / MEMBERS)
            for tile in tiles:
                deviation = tile - mean
                total = total + deviation * deviation
    acc = jnp.concatenate([total, jnp.zeros((128 - DEGREES, 128), jnp.float32)], axis=0)
    squares[...] = jnp.broadcast_to(jnp.sum(acc.T, axis=0, keepdims=True), (8, 128))

    @pl.loop(1, LON)
    def _(i):
        d = lon_peer(i)
        pltpu.make_async_remote_copy(
            src_ref=squares,
            dst_ref=all_squares.at[g],
            send_sem=sq_send,
            recv_sem=sq_recv,
            device_id={"lon": d},
            device_id_type=MESH,
        ).start()

    pltpu.make_async_copy(squares, all_squares.at[g], sq_recv).start()
    wait_bytes(all_squares, sq_recv)
    summed = all_squares[0]
    for i in range(1, LON):
        summed = summed + all_squares[i]
    degree = (b * DEGREES + lax.broadcasted_iota(jnp.int32, (8, 128), 1)).astype(jnp.float32)
    spread = summed / ((MEMBERS - 1) * CHANNELS * (2.0 * degree + 1.0))
    spread_ref[...] = spread
    scale = lax.rsqrt(spread + EPSILON)
    scale = jnp.broadcast_to(scale[0:1], (128, 128)).T
    for block in range(3):
        rows = scale[16 * block : 16 * (block + 1)]
        rows = jnp.concatenate([rows, rows, rows], axis=1)
        x = coeffs[:, :, 16 * block : 16 * (block + 1), :].reshape(2 * ORDERS, 16, FIELDS).astype(jnp.float32)
        y = (x * rows[None]).astype(jnp.bfloat16).reshape(2 * ORDERS * 16, FIELDS)
        moved = jnp.dot(swap_out[...], y, preferred_element_type=jnp.float32)
        out_ref[16 * block : 16 * (block + 1)] = moved.reshape(16, 2 * ORDERS, FIELDS).astype(jnp.bfloat16)

    for chunk in range(CHUNKS):
        if chunk < 2:
            wait_bytes(recv.at[chunk, pl.ds(0, LON - 1)], grid_send.at[chunk])
        else:

            @pl.when(has_row(chunk, g))
            def _():
                wait_bytes(recv.at[chunk, pl.ds(0, 25)], grid_send.at[chunk])

            @pl.when(jnp.logical_not(has_row(chunk, g)))
            def _():
                wait_bytes(recv.at[chunk, pl.ds(0, 26)], grid_send.at[chunk])

        @pl.when(has_row(chunk, g))
        def _():
            wait_bytes(mixed.at[chunk, pl.ds(0, LAT - 1)], mix_send.at[chunk])
            wait_bytes(sent.at[chunk, pl.ds(0, UNITS * (LON - 1))], spec_send.at[chunk])

    wait_bytes(leg_raw.at[pl.ds(0, LAT - 1)], leg_send)
    wait_bytes(coeffs.at[pl.ds(0, LAT - 1)], coef_send)
    wait_bytes(all_squares.at[pl.ds(0, LON - 1)], sq_send)


def shards(grid, legendre):
    padded = jnp.pad(grid, ((0, 0), (0, PADDED - LON_ROWS), (0, 0)))
    basis = jnp.asarray(spectral_table())
    dma = pltpu.SemaphoreType.DMA
    bf16, f32 = jnp.bfloat16, jnp.float32
    any_space = pl.BlockSpec(memory_space=pl.ANY)
    vmem = pl.BlockSpec(memory_space=pltpu.VMEM)
    normalized, spread = pl.pallas_call(
        kernel,
        out_shape=(
            jax.ShapeDtypeStruct((DEGREES, 2 * ORDERS, FIELDS), bf16),
            jax.ShapeDtypeStruct((8, 128), f32),
        ),
        in_specs=[any_space, any_space, any_space],
        out_specs=(vmem, vmem),
        scratch_shapes=[
            pltpu.VMEM((CHUNKS, LON, PADDED, FIELDS), bf16),
            pltpu.VMEM((2 * DEG, LON * PADDED), bf16),
            pltpu.VMEM((CHUNKS, LAT, LON * UNITS, FIELDS), bf16),
            pltpu.VMEM((CHUNKS, LAT, LON * UNITS, FIELDS), bf16),
            pltpu.VMEM((CHUNKS, LON * UNITS, LAT, FIELDS), bf16),
            pltpu.VMEM((UNITS, JPAD, LAT, FIELDS), bf16),
            pltpu.VMEM((LAT, 2, ROWS, DEG), bf16),
            pltpu.VMEM((2, DEG, JPAD * LAT), bf16),
            pltpu.VMEM((LAT, UNITS, DEGREES, FIELDS), bf16),
            pltpu.VMEM((LAT, UNITS, DEGREES, FIELDS), bf16),
            pltpu.VMEM((8, 128), f32),
            pltpu.VMEM((LON, 8, 128), f32),
            pltpu.VMEM((256, 256), bf16),
            pltpu.VMEM((128, 128), bf16),
            pltpu.VMEM((384, 384), bf16),
            dma,
            dma((CHUNKS,)),
            dma((CHUNKS,)),
            dma,
            dma,
            dma((CHUNKS,)),
            dma((CHUNKS,)),
            dma((CHUNKS,)),
            dma,
            dma,
            dma,
            dma,
            dma,
        ],
        compiler_params=pltpu.CompilerParams(
            collective_id=0, has_side_effects=True, vmem_limit_bytes=48 * 1024 * 1024
        ),
        cost_estimate=pl.CostEstimate(flops=4_000_000_000, bytes_accessed=8_000_000, transcendentals=0),
    )(padded, legendre, basis)
    return normalized.reshape(DEGREES, ORDERS, 2, FIELDS), spread[0, :DEGREES]


def solution(mesh):
    return jax.shard_map(
        shards,
        mesh=mesh,
        in_specs=(P("lat", "lon", None), P("lon", "lat", None)),
        out_specs=(P("lat", "lon", None, None), P("lat")),
        check_vma=False,
    )
```

```python
import math

import jax
import jax.numpy as jnp
import numpy as np
from jax import lax
from jax.experimental import pallas as pl
from jax.experimental.pallas import tpu as pltpu
from jax.sharding import PartitionSpec as P

NLON = 1440
DEG = 384
CHANNELS = 64
MEMBERS = 6
FIELDS = 384
LAT = 8
LON = 32
ROWS = 90
LON_ROWS = 45
MAIN = 40
REST = LON_ROWS - MAIN
REST_PAD = 16
ORDERS = 12
DEGREES = 48
UNITS = 3
CHUNKS = 3
JPAD = 96
EPSILON = 1e-06
MESH = pl.DeviceIdType.MESH


def spectral_table():
    k = np.arange(NLON, dtype=np.int64)[:, None]
    m = np.arange(DEG, dtype=np.int64)[None, :]
    angle = ((k * m) % NLON).astype(np.float32) * np.float32(2.0 * math.pi / NLON)
    table = np.stack([np.cos(angle), -np.sin(angle)], axis=2).astype(np.float32)
    table = table.reshape(LON, LON_ROWS, LON, LAT, UNITS)
    table = table.transpose(3, 2, 4, 0, 1).reshape(2 * DEG, LON, LON_ROWS)
    rest = np.zeros((2 * DEG, LON, REST_PAD), np.float32)
    rest[:, :, :REST] = table[:, :, MAIN:]
    main = table[:, :, :MAIN].reshape(2 * DEG, LON * MAIN)
    return main.astype(jnp.bfloat16), rest.reshape(2 * DEG, LON * REST_PAD).astype(jnp.bfloat16)


def wait_bytes(ref, sem):
    pltpu.make_async_copy(ref, ref, sem).wait()


def swap_matrix(major, minor):
    size = major * minor
    out_row = lax.broadcasted_iota(jnp.int32, (size, size), 0)
    in_row = lax.broadcasted_iota(jnp.int32, (size, size), 1)
    wanted = (out_row % major) * minor + out_row // major
    return (in_row == wanted).astype(jnp.float32).astype(jnp.bfloat16)


def kernel(
    grid_ref,
    leg_ref,
    main_ref,
    rest_ref,
    out_ref,
    spread_ref,
    recv,
    rest_raw,
    rest_out,
    rest_in,
    basis,
    rest_basis,
    spec,
    mixed,
    sent,
    spectral,
    leg_raw,
    leg,
    begun,
    part,
    coeffs,
    turned,
    squares,
    all_squares,
    swap_spec,
    swap_leg,
    swap_out,
    basis_sem,
    raw_sem,
    grid_send,
    grid_recv,
    rest_send,
    rest_recv,
    leg_send,
    leg_recv,
    mix_send,
    mix_recv,
    spec_send,
    spec_recv,
    last_recv,
    coef_send,
    coef_recv,
    sq_send,
    sq_recv,
):
    b = lax.axis_index("lat")
    g = lax.axis_index("lon")

    def lon_peer(i):
        return (g + i) % LON

    def lat_peer(i):
        return (b + i) % LAT

    def has_row(chunk, d):
        return (chunk < 2) | (d % 5 != 4)

    def row_of(chunk, d):
        return chunk * LON + d - jnp.where(chunk == 2, d // 5, 0)

    def to_lon(src, dst, send_sem, recv_sem, d):
        pltpu.make_async_remote_copy(
            src_ref=src, dst_ref=dst, send_sem=send_sem, recv_sem=recv_sem, device_id={"lon": d}, device_id_type=MESH
        ).start()

    def to_lat(src, dst, send_sem, recv_sem, d):
        pltpu.make_async_remote_copy(
            src_ref=src, dst_ref=dst, send_sem=send_sem, recv_sem=recv_sem, device_id={"lat": d}, device_id_type=MESH
        ).start()

    raw_copy = pltpu.make_async_copy(grid_ref.at[:, pl.ds(MAIN, REST)], rest_raw, raw_sem)
    raw_copy.start()
    basis_copy = pltpu.make_async_copy(main_ref, basis, basis_sem.at[0])
    basis_copy.start()
    first_rest_copy = pltpu.make_async_copy(rest_ref, rest_basis.at[0], basis_sem.at[1])
    first_rest_copy.start()
    barrier = pltpu.get_barrier_semaphore()

    @pl.loop(1, LON)
    def _(i):
        pl.semaphore_signal(barrier, inc=1, device_id={"lon": lon_peer(i)}, device_id_type=MESH)

    @pl.loop(1, LAT)
    def _(i):
        pl.semaphore_signal(barrier, inc=1, device_id={"lat": lat_peer(i)}, device_id_type=MESH)

    raw_copy.wait()

    @pl.loop(0, LON)
    def _(d):
        pieces = [rest_raw[row_of(chunk, d)].astype(jnp.float32) for chunk in range(2)]
        last = rest_raw[jnp.minimum(row_of(2, d), ROWS - 1)].astype(jnp.float32)
        pieces += [jnp.where(has_row(2, d), last, 0.0), jnp.zeros((1, FIELDS), jnp.float32)]
        rest_out[d] = jnp.concatenate(pieces, axis=0).astype(jnp.bfloat16)

    pl.semaphore_wait(barrier, LON + LAT - 2)

    @pl.loop(1, LAT)
    def _(i):
        u = lat_peer(i)
        to_lat(leg_ref.at[pl.ds(UNITS * u // 2, 2)], leg_raw.at[b], leg_send, leg_recv, u)

    pltpu.make_async_copy(leg_ref.at[pl.ds(UNITS * b // 2, 2)], leg_raw.at[b], leg_recv).start()

    @pl.loop(1, LON)
    def _(i):
        d = lon_peer(i)
        to_lon(rest_out.at[d], rest_in.at[g], rest_send, rest_recv, d)

    pltpu.make_async_copy(rest_out.at[g], rest_in.at[g], rest_recv).start()

    @pl.loop(0, CHUNKS)
    def _(chunk):
        @pl.loop(1, LON)
        def _(i):
            d = lon_peer(i)

            @pl.when(has_row(chunk, d))
            def _():
                src = grid_ref.at[row_of(chunk, d), pl.ds(0, MAIN)]
                to_lon(src, recv.at[chunk, g], grid_send.at[chunk], grid_recv.at[chunk], d)

        @pl.when(has_row(chunk, g))
        def _():
            src = grid_ref.at[row_of(chunk, g), pl.ds(0, MAIN)]
            pltpu.make_async_copy(src, recv.at[chunk, g], grid_recv.at[chunk]).start()

    swap_spec[...] = swap_matrix(LAT, 32)
    swap_leg[...] = swap_matrix(LAT, 16)
    swap_out[...] = swap_matrix(2 * ORDERS, 16)
    spectral[:, ROWS:] = jnp.zeros((UNITS, JPAD - ROWS, LAT, FIELDS), spectral.dtype)

    first_rest_copy.wait()
    size = LON * REST_PAD
    from_column = lax.broadcasted_iota(jnp.int32, (size, size), 0)
    to_column = lax.broadcasted_iota(jnp.int32, (size, size), 1)
    for chunk in range(1, CHUNKS):
        move = (from_column + REST * chunk == to_column).astype(jnp.float32).astype(jnp.bfloat16)
        moved = jnp.dot(rest_basis[0], move, preferred_element_type=jnp.float32)
        rest_basis[chunk] = moved.astype(jnp.bfloat16)

    wait_bytes(leg_raw, leg_recv)
    for which in range(2):
        for block in range(JPAD // 16):
            first = 16 * block
            rows = min(16, ROWS - first)
            piece = leg_raw[:, which, first : first + rows, :].astype(jnp.float32)
            if rows < 16:
                piece = jnp.concatenate([piece, jnp.zeros((LAT, 16 - rows, DEG), jnp.float32)], axis=1)
            piece = piece.reshape(LAT * 16, DEG).astype(jnp.bfloat16)
            moved = jnp.dot(swap_leg[...], piece, preferred_element_type=jnp.float32)
            leg[which, :, 128 * block : 128 * (block + 1)] = moved.T.astype(jnp.bfloat16)

    def send_spectrum(chunk):
        row = row_of(chunk, g)

        @pl.loop(1, LON)
        def _(i):
            d = lon_peer(i)
            src = sent.at[chunk, pl.ds(UNITS * d, UNITS)]
            to_lon(src, spectral.at[:, row], spec_send.at[chunk], spec_recv, d)

        pltpu.make_async_copy(sent.at[chunk, pl.ds(UNITS * g, UNITS)], spectral.at[:, row], spec_recv).start()

    def send_last():
        row = row_of(2, g)
        for unit in range(UNITS):

            @pl.loop(1, LON)
            def _(i):
                d = lon_peer(i)
                src = sent.at[2, UNITS * d + unit]
                to_lon(src, spectral.at[unit, row], spec_send.at[2], last_recv.at[unit], d)

            pltpu.make_async_copy(sent.at[2, UNITS * g + unit], spectral.at[unit, row], last_recv.at[unit]).start()

    basis_copy.wait()
    wait_bytes(rest_in, rest_recv)

    @pl.loop(0, CHUNKS)
    def _(chunk):
        @pl.when(has_row(chunk, g))
        def _():
            wait_bytes(recv.at[chunk], grid_recv.at[chunk])
            values = recv[chunk].astype(jnp.float32).reshape(LON * MAIN, FIELDS).astype(jnp.bfloat16)
            rows = jnp.dot(basis[...], values, preferred_element_type=jnp.float32)
            values = rest_in[...].reshape(LON * REST_PAD, FIELDS)
            rows = rows + jnp.dot(rest_basis[chunk], values, preferred_element_type=jnp.float32)
            spec[chunk] = rows.astype(jnp.bfloat16).reshape(LAT, LON * UNITS, FIELDS)

            @pl.loop(1, LAT)
            def _(i):
                u = lat_peer(i)
                to_lat(spec.at[chunk, u], mixed.at[chunk, b], mix_send.at[chunk], mix_recv.at[chunk], u)

            pltpu.make_async_copy(spec.at[chunk, b], mixed.at[chunk, b], mix_recv.at[chunk]).start()
            wait_bytes(mixed.at[chunk], mix_recv.at[chunk])
            for block in range(3):
                piece = mixed[chunk, :, 32 * block : 32 * (block + 1), :].reshape(LAT * 32, FIELDS)
                moved = jnp.dot(swap_spec[...], piece, preferred_element_type=jnp.float32)
                sent[chunk, 32 * block : 32 * (block + 1)] = moved.reshape(32, LAT, FIELDS).astype(jnp.bfloat16)
            pl.when(chunk < 2)(lambda: send_spectrum(chunk))
            pl.when(chunk == 2)(send_last)

    early = 2 * LON
    wait_bytes(spectral.at[:, pl.ds(0, early)], spec_recv)

    def table_of(unit):
        return (UNITS * b + unit) // 2 - UNITS * b // 2

    for unit in range(UNITS):
        values = spectral[unit, :early].astype(jnp.float32).reshape(early * LAT, FIELDS).astype(jnp.bfloat16)
        begun[unit] = jnp.dot(leg[table_of(unit), :, : early * LAT], values, preferred_element_type=jnp.float32)
    for unit in range(UNITS):
        wait_bytes(spectral.at[unit, pl.ds(early, ROWS - early)], last_recv.at[unit])
        values = spectral[unit, early:].astype(jnp.float32).reshape((JPAD - early) * LAT, FIELDS).astype(jnp.bfloat16)
        total = jnp.dot(leg[table_of(unit), :, early * LAT :], values, preferred_element_type=jnp.float32)
        total = begun[unit] + total
        part[:, unit] = total.astype(jnp.bfloat16).reshape(LAT, DEGREES, FIELDS)

        @pl.loop(1, LAT)
        def _(i):
            u = lat_peer(i)
            to_lat(part.at[u, unit], coeffs.at[b, unit], coef_send, coef_recv.at[unit], u)

        pltpu.make_async_copy(part.at[b, unit], coeffs.at[b, unit], coef_recv.at[unit]).start()

    total = jnp.zeros((DEGREES, 128), jnp.float32)
    for unit in range(UNITS):
        wait_bytes(coeffs.at[:, unit], coef_recv.at[unit])
        for u in range(LAT):
            x = coeffs[u, unit].astype(jnp.float32)
            tiles = [x[:, 128 * t : 128 * (t + 1)] for t in range(3)]
            both = tiles[0] + tiles[1] + tiles[2]
            mean = (both + pltpu.roll(both, CHANNELS, 1)) * (1.0 / MEMBERS)
            for tile in tiles:
                deviation = tile - mean
                total = total + deviation * deviation
    acc = jnp.concatenate([total, jnp.zeros((128 - DEGREES, 128), jnp.float32)], axis=0)
    squares[...] = jnp.sum(acc.T, axis=0, keepdims=True)

    @pl.loop(1, LON)
    def _(i):
        to_lon(squares, all_squares.at[g], sq_send, sq_recv, lon_peer(i))

    pltpu.make_async_copy(squares, all_squares.at[g], sq_recv).start()
    for block in range(3):
        x = coeffs[:, :, 16 * block : 16 * (block + 1), :].reshape(2 * ORDERS * 16, FIELDS)
        moved = jnp.dot(swap_out[...], x, preferred_element_type=jnp.float32)
        turned[16 * block : 16 * (block + 1)] = moved.reshape(16, 2 * ORDERS, FIELDS)

    wait_bytes(all_squares, sq_recv)
    summed = all_squares[0]
    for i in range(1, LON):
        summed = summed + all_squares[i]
    degree = (b * DEGREES + lax.broadcasted_iota(jnp.int32, (1, 128), 1)).astype(jnp.float32)
    spread = summed / ((MEMBERS - 1) * CHANNELS * (2.0 * degree + 1.0))
    spread_ref[...] = jnp.broadcast_to(spread, (8, 128))
    scale = jnp.broadcast_to(lax.rsqrt(spread + EPSILON), (128, 128)).T
    scale = jnp.concatenate([scale[:DEGREES]] * 3, axis=1)
    for degree in range(DEGREES):
        out_ref[degree] = (turned[degree] * scale[degree : degree + 1]).astype(jnp.bfloat16)

    for chunk in range(CHUNKS):
        if chunk < 2:
            wait_bytes(recv.at[chunk, pl.ds(0, LON - 1)], grid_send.at[chunk])
        else:

            @pl.when(has_row(chunk, g))
            def _():
                wait_bytes(recv.at[chunk, pl.ds(0, 25)], grid_send.at[chunk])

            @pl.when(jnp.logical_not(has_row(chunk, g)))
            def _():
                wait_bytes(recv.at[chunk, pl.ds(0, 26)], grid_send.at[chunk])

        @pl.when(has_row(chunk, g))
        def _():
            wait_bytes(mixed.at[chunk, pl.ds(0, LAT - 1)], mix_send.at[chunk])
            wait_bytes(sent.at[chunk, pl.ds(0, UNITS * (LON - 1))], spec_send.at[chunk])

    wait_bytes(rest_in.at[pl.ds(0, LON - 1)], rest_send)
    wait_bytes(leg_raw.at[pl.ds(0, LAT - 1)], leg_send)
    wait_bytes(coeffs.at[pl.ds(0, LAT - 1)], coef_send)
    wait_bytes(all_squares.at[pl.ds(0, LON - 1)], sq_send)


def shards(grid, legendre):
    main, rest = [jnp.asarray(table) for table in spectral_table()]
    dma = pltpu.SemaphoreType.DMA
    bf16, f32 = jnp.bfloat16, jnp.float32
    any_space = pl.BlockSpec(memory_space=pl.ANY)
    vmem = pl.BlockSpec(memory_space=pltpu.VMEM)
    normalized, spread = pl.pallas_call(
        kernel,
        out_shape=(
            jax.ShapeDtypeStruct((DEGREES, 2 * ORDERS, FIELDS), bf16),
            jax.ShapeDtypeStruct((8, 128), f32),
        ),
        in_specs=[any_space] * 4,
        out_specs=(vmem, vmem),
        scratch_shapes=[
            pltpu.VMEM((CHUNKS, LON, MAIN, FIELDS), bf16),
            pltpu.VMEM((ROWS, REST, FIELDS), bf16),
            pltpu.VMEM((LON, REST_PAD, FIELDS), bf16),
            pltpu.VMEM((LON, REST_PAD, FIELDS), bf16),
            pltpu.VMEM((2 * DEG, LON * MAIN), bf16),
            pltpu.VMEM((CHUNKS, 2 * DEG, LON * REST_PAD), bf16),
            pltpu.VMEM((CHUNKS, LAT, LON * UNITS, FIELDS), bf16),
            pltpu.VMEM((CHUNKS, LAT, LON * UNITS, FIELDS), bf16),
            pltpu.VMEM((CHUNKS, LON * UNITS, LAT, FIELDS), bf16),
            pltpu.VMEM((UNITS, JPAD, LAT, FIELDS), bf16),
            pltpu.VMEM((LAT, 2, ROWS, DEG), bf16),
            pltpu.VMEM((2, DEG, JPAD * LAT), bf16),
            pltpu.VMEM((UNITS, DEG, FIELDS), f32),
            pltpu.VMEM((LAT, UNITS, DEGREES, FIELDS), bf16),
            pltpu.VMEM((LAT, UNITS, DEGREES, FIELDS), bf16),
            pltpu.VMEM((DEGREES, 2 * ORDERS, FIELDS), f32),
            pltpu.VMEM((1, 128), f32),
            pltpu.VMEM((LON, 1, 128), f32),
            pltpu.VMEM((256, 256), bf16),
            pltpu.VMEM((128, 128), bf16),
            pltpu.VMEM((384, 384), bf16),
            dma((2,)),
            dma,
            dma((CHUNKS,)),
            dma((CHUNKS,)),
            dma,
            dma,
            dma,
            dma,
            dma((CHUNKS,)),
            dma((CHUNKS,)),
            dma((CHUNKS,)),
            dma,
            dma((UNITS,)),
            dma,
            dma((UNITS,)),
            dma,
            dma,
        ],
        compiler_params=pltpu.CompilerParams(
            collective_id=0, has_side_effects=True, vmem_limit_bytes=48 * 1024 * 1024
        ),
        cost_estimate=pl.CostEstimate(flops=4_000_000_000, bytes_accessed=8_000_000, transcendentals=0),
    )(*[pltpu.with_memory_space_constraint(x, pltpu.HBM) for x in (grid, legendre, main, rest)])
    return normalized.reshape(DEGREES, ORDERS, 2, FIELDS), spread[0, :DEGREES]


def solution(mesh):
    return jax.shard_map(
        shards,
        mesh=mesh,
        in_specs=(P("lat", "lon", None), P("lon", "lat", None)),
        out_specs=(P("lat", "lon", None, None), P("lat")),
        check_vma=False,
    )
```

```python
import functools
import math

import jax
import jax.numpy as jnp
import numpy as np
from jax import lax
from jax.experimental import pallas as pl
from jax.experimental.pallas import tpu as pltpu
from jax.sharding import PartitionSpec as P

NLON = 1440
DEG = 384
CHANNELS = 64
MEMBERS = 6
FIELDS = 384
LAT = 8
LON = 32
ROWS = 90
LON_ROWS = 45
MAIN = 40
REST = LON_ROWS - MAIN
REST_PAD = 16
ORDERS = 12
DEGREES = 48
UNITS = 3
CHUNKS = 3
JPAD = 96
EPSILON = 1e-06
MESH = pl.DeviceIdType.MESH


def spectral_table():
    k = np.arange(NLON, dtype=np.int64)[:, None]
    m = np.arange(DEG, dtype=np.int64)[None, :]
    angle = ((k * m) % NLON).astype(np.float32) * np.float32(2.0 * math.pi / NLON)
    table = np.stack([np.cos(angle), -np.sin(angle)], axis=2).astype(np.float32)
    table = table.reshape(LON, LON_ROWS, LON, LAT, UNITS)
    table = table.transpose(3, 2, 4, 0, 1).reshape(2 * DEG, LON, LON_ROWS)
    rest = np.zeros((2 * DEG, LON, REST_PAD), np.float32)
    rest[:, :, :REST] = table[:, :, MAIN:]
    main = table[:, :, :MAIN].reshape(2 * DEG, LON * MAIN)
    return main.astype(jnp.bfloat16), rest.reshape(2 * DEG, LON * REST_PAD).astype(jnp.bfloat16)


def wait_bytes(ref, sem):
    pltpu.make_async_copy(ref, ref, sem).wait()


def swap_matrix(major, minor):
    size = major * minor
    out_row = lax.broadcasted_iota(jnp.int32, (size, size), 0)
    in_row = lax.broadcasted_iota(jnp.int32, (size, size), 1)
    wanted = (out_row % major) * minor + out_row // major
    return (in_row == wanted).astype(jnp.float32).astype(jnp.bfloat16)


def kernel(
    grid_ref,
    leg_ref,
    main_ref,
    rest_ref,
    out_ref,
    spread_ref,
    recv,
    rest_raw,
    rest_out,
    rest_in,
    basis,
    rest_basis,
    spec,
    mixed,
    sent,
    spectral,
    leg_raw,
    leg,
    begun,
    part,
    coeffs,
    turned,
    by_degree,
    squares,
    all_squares,
    unit_squares,
    all_units,
    swap_spec,
    swap_leg,
    swap_out,
    basis_sem,
    raw_sem,
    grid_send,
    grid_recv,
    rest_send,
    rest_recv,
    leg_send,
    leg_recv,
    mix_send,
    mix_recv,
    spec_send,
    spec_recv,
    last_recv,
    coef_send,
    coef_recv,
    sq_send,
    sq_recv,
    unit_send,
    unit_recv,
):
    b = lax.axis_index("lat")
    g = lax.axis_index("lon")

    def lon_peer(i):
        return (g + i) % LON

    def lat_peer(i):
        return (b + i) % LAT

    def first_piece(d):
        return 39 * d // 16

    def has_piece(d, k):
        return first_piece(d) + k < first_piece(d + 1)

    def piece_of(d, k):
        piece = first_piece(d) + k
        return 2 * LON + piece // 3, pl.ds(pl.multiple_of(128 * (piece % 3), 128), 128)

    def each_piece(d, action):
        for k in range(CHUNKS):
            row, fields = piece_of(d, k)
            run = functools.partial(action, row, fields, pl.ds(128 * k, 128))
            if k < 2:
                run()
            else:
                pl.when(has_piece(d, k))(run)

    def to_lon(src, dst, send_sem, recv_sem, d):
        pltpu.make_async_remote_copy(
            src_ref=src, dst_ref=dst, send_sem=send_sem, recv_sem=recv_sem, device_id={"lon": d}, device_id_type=MESH
        ).start()

    def to_lat(src, dst, send_sem, recv_sem, d):
        pltpu.make_async_remote_copy(
            src_ref=src, dst_ref=dst, send_sem=send_sem, recv_sem=recv_sem, device_id={"lat": d}, device_id_type=MESH
        ).start()

    raw_copy = pltpu.make_async_copy(grid_ref.at[:, pl.ds(MAIN, REST)], rest_raw, raw_sem)
    raw_copy.start()
    basis_copy = pltpu.make_async_copy(main_ref, basis, basis_sem.at[0])
    basis_copy.start()
    first_rest_copy = pltpu.make_async_copy(rest_ref, rest_basis.at[0], basis_sem.at[1])
    first_rest_copy.start()
    barrier = pltpu.get_barrier_semaphore()

    @pl.loop(1, LON)
    def _(i):
        pl.semaphore_signal(barrier, inc=1, device_id={"lon": lon_peer(i)}, device_id_type=MESH)

    @pl.loop(1, LAT)
    def _(i):
        pl.semaphore_signal(barrier, inc=1, device_id={"lat": lat_peer(i)}, device_id_type=MESH)

    pl.semaphore_wait(barrier, LON + LAT - 2)

    def send_rows(chunk):
        @pl.loop(1, LON)
        def _(i):
            d = lon_peer(i)
            src = grid_ref.at[chunk * LON + d, pl.ds(0, MAIN)]
            to_lon(src, recv.at[chunk, g], grid_send.at[chunk], grid_recv.at[chunk], d)

        src = grid_ref.at[chunk * LON + g, pl.ds(0, MAIN)]
        pltpu.make_async_copy(src, recv.at[chunk, g], grid_recv.at[chunk]).start()

    send_rows(0)

    @pl.loop(1, LAT)
    def _(i):
        u = lat_peer(i)
        to_lat(leg_ref.at[pl.ds(UNITS * u // 2, 2)], leg_raw.at[b], leg_send, leg_recv, u)

    pltpu.make_async_copy(leg_ref.at[pl.ds(UNITS * b // 2, 2)], leg_raw.at[b], leg_recv).start()

    raw_copy.wait()

    @pl.loop(0, LON)
    def _(d):
        pieces = [rest_raw[d].astype(jnp.float32), rest_raw[LON + d].astype(jnp.float32)]
        last = []
        for k in range(CHUNKS):
            row, fields = piece_of(d, k)
            last.append(rest_raw[row, :, fields].astype(jnp.float32))
        last[2] = jnp.where(has_piece(d, 2), last[2], 0.0)
        pieces += [jnp.concatenate(last, axis=1), jnp.zeros((1, FIELDS), jnp.float32)]
        rest_out[d] = jnp.concatenate(pieces, axis=0).astype(jnp.bfloat16)

    @pl.loop(1, LON)
    def _(i):
        d = lon_peer(i)
        to_lon(rest_out.at[d], rest_in.at[g], rest_send, rest_recv, d)

    pltpu.make_async_copy(rest_out.at[g], rest_in.at[g], rest_recv).start()
    send_rows(1)

    @pl.loop(1, LON)
    def _(i):
        d = lon_peer(i)

        def send(row, fields, lanes):
            src = grid_ref.at[row, pl.ds(0, MAIN), fields]
            to_lon(src, recv.at[2, g, :, lanes], grid_send.at[2], grid_recv.at[2], d)

        each_piece(d, send)

    def keep(row, fields, lanes):
        src = grid_ref.at[row, pl.ds(0, MAIN), fields]
        pltpu.make_async_copy(src, recv.at[2, g, :, lanes], grid_recv.at[2]).start()

    each_piece(g, keep)

    @pl.when(jnp.logical_not(has_piece(g, 2)))
    def _():
        recv[2, :, :, 256:] = jnp.zeros((LON, MAIN, 128), recv.dtype)

    swap_spec[...] = swap_matrix(LAT, 32)
    swap_leg[...] = swap_matrix(LAT, 16)
    swap_out[...] = swap_matrix(2 * ORDERS, 16)
    spectral[:, ROWS:] = jnp.zeros((UNITS, JPAD - ROWS, LAT, FIELDS), spectral.dtype)

    first_rest_copy.wait()
    size = LON * REST_PAD
    from_column = lax.broadcasted_iota(jnp.int32, (size, size), 0)
    to_column = lax.broadcasted_iota(jnp.int32, (size, size), 1)
    for chunk in range(1, CHUNKS):
        move = (from_column + REST * chunk == to_column).astype(jnp.float32).astype(jnp.bfloat16)
        moved = jnp.dot(rest_basis[0], move, preferred_element_type=jnp.float32)
        rest_basis[chunk] = moved.astype(jnp.bfloat16)

    wait_bytes(leg_raw, leg_recv)
    for which in range(2):
        for block in range(JPAD // 16):
            first = 16 * block
            rows = min(16, ROWS - first)
            piece = leg_raw[:, which, first : first + rows, :].astype(jnp.float32)
            if rows < 16:
                piece = jnp.concatenate([piece, jnp.zeros((LAT, 16 - rows, DEG), jnp.float32)], axis=1)
            piece = piece.reshape(LAT * 16, DEG).astype(jnp.bfloat16)
            moved = jnp.dot(swap_leg[...], piece, preferred_element_type=jnp.float32)
            leg[which, :, 128 * block : 128 * (block + 1)] = moved.T.astype(jnp.bfloat16)

    def send_spectrum(chunk):
        row = chunk * LON + g

        @pl.loop(1, LON)
        def _(i):
            d = lon_peer(i)
            src = sent.at[chunk, pl.ds(UNITS * d, UNITS)]
            to_lon(src, spectral.at[:, row], spec_send.at[chunk], spec_recv, d)

        pltpu.make_async_copy(sent.at[chunk, pl.ds(UNITS * g, UNITS)], spectral.at[:, row], spec_recv).start()

    def send_last():
        for unit in range(UNITS):

            @pl.loop(1, LON)
            def _(i):
                d = lon_peer(i)

                def send(row, fields, lanes):
                    src = sent.at[2, UNITS * d + unit, :, lanes]
                    to_lon(src, spectral.at[unit, row, :, fields], spec_send.at[2], last_recv.at[unit], d)

                each_piece(g, send)

            def keep(row, fields, lanes):
                src = sent.at[2, UNITS * g + unit, :, lanes]
                pltpu.make_async_copy(src, spectral.at[unit, row, :, fields], last_recv.at[unit]).start()

            each_piece(g, keep)

    basis_copy.wait()
    wait_bytes(rest_in, rest_recv)

    @pl.loop(0, CHUNKS)
    def _(chunk):
        @pl.when((chunk < 2) | has_piece(g, 2))
        def _():
            wait_bytes(recv.at[chunk], grid_recv.at[chunk])

        @pl.when((chunk == 2) & jnp.logical_not(has_piece(g, 2)))
        def _():
            wait_bytes(recv.at[chunk, :, :, pl.ds(0, 256)], grid_recv.at[chunk])

        values = recv[chunk].astype(jnp.float32).reshape(LON * MAIN, FIELDS).astype(jnp.bfloat16)
        rows = jnp.dot(basis[...], values, preferred_element_type=jnp.float32)
        values = rest_in[...].reshape(LON * REST_PAD, FIELDS)
        rows = rows + jnp.dot(rest_basis[chunk], values, preferred_element_type=jnp.float32)
        spec[chunk] = rows.astype(jnp.bfloat16).reshape(LAT, LON * UNITS, FIELDS)

        @pl.loop(1, LAT)
        def _(i):
            u = lat_peer(i)
            to_lat(spec.at[chunk, u], mixed.at[chunk, b], mix_send.at[chunk], mix_recv.at[chunk], u)

        pltpu.make_async_copy(spec.at[chunk, b], mixed.at[chunk, b], mix_recv.at[chunk]).start()
        wait_bytes(mixed.at[chunk], mix_recv.at[chunk])
        for block in range(3):
            piece = mixed[chunk, :, 32 * block : 32 * (block + 1), :].reshape(LAT * 32, FIELDS)
            moved = jnp.dot(swap_spec[...], piece, preferred_element_type=jnp.float32)
            sent[chunk, 32 * block : 32 * (block + 1)] = moved.reshape(32, LAT, FIELDS).astype(jnp.bfloat16)
        pl.when(chunk < 2)(lambda: send_spectrum(chunk))
        pl.when(chunk == 2)(send_last)

    early = 2 * LON
    wait_bytes(spectral.at[:, pl.ds(0, early)], spec_recv)

    def table_of(unit):
        return (UNITS * b + unit) // 2 - UNITS * b // 2

    for unit in range(UNITS):
        values = spectral[unit, :early].astype(jnp.float32).reshape(early * LAT, FIELDS).astype(jnp.bfloat16)
        begun[unit] = jnp.dot(leg[table_of(unit), :, : early * LAT], values, preferred_element_type=jnp.float32)
    for unit in range(UNITS):
        wait_bytes(spectral.at[unit, pl.ds(early, ROWS - early)], last_recv.at[unit])
        values = spectral[unit, early:].astype(jnp.float32).reshape((JPAD - early) * LAT, FIELDS).astype(jnp.bfloat16)
        total = jnp.dot(leg[table_of(unit), :, early * LAT :], values, preferred_element_type=jnp.float32)
        total = begun[unit] + total
        part[:, unit] = total.astype(jnp.bfloat16).reshape(LAT, DEGREES, FIELDS)

        @pl.loop(1, LAT)
        def _(i):
            u = lat_peer(i)
            to_lat(part.at[u, unit], coeffs.at[b, unit], coef_send, coef_recv, u)

        pltpu.make_async_copy(part.at[b, unit], coeffs.at[b, unit], coef_recv).start()
        tiles = [total[:, 128 * t : 128 * (t + 1)] for t in range(3)]
        both = tiles[0] + tiles[1] + tiles[2]
        mean = (both + pltpu.roll(both, CHANNELS, 1)) * (1.0 / MEMBERS)
        square = sum((tile - mean) * (tile - mean) for tile in tiles)
        by_degree[...] = square if unit == 0 else by_degree[...] + square

    for third in range(3):
        rows = by_degree[128 * third : 128 * (third + 1)]
        squares[third : third + 1] = jnp.sum(rows.T, axis=0, keepdims=True)

    @pl.loop(1, LON)
    def _(i):
        to_lon(squares, all_squares.at[g], sq_send, sq_recv, lon_peer(i))

    pltpu.make_async_copy(squares, all_squares.at[g], sq_recv).start()
    wait_bytes(all_squares, sq_recv)
    summed = all_squares[0]
    for i in range(1, LON):
        summed = summed + all_squares[i]
    unit_squares[...] = summed

    @pl.loop(1, LAT)
    def _(i):
        to_lat(unit_squares, all_units.at[b], unit_send, unit_recv, lat_peer(i))

    pltpu.make_async_copy(unit_squares, all_units.at[b], unit_recv).start()
    wait_bytes(coeffs, coef_recv)
    for block in range(3):
        x = coeffs[:, :, 16 * block : 16 * (block + 1), :].reshape(2 * ORDERS * 16, FIELDS)
        moved = jnp.dot(swap_out[...], x, preferred_element_type=jnp.float32)
        turned[16 * block : 16 * (block + 1)] = moved.reshape(16, 2 * ORDERS, FIELDS)

    wait_bytes(all_units, unit_recv)
    summed = all_units[0]
    for i in range(1, LAT):
        summed = summed + all_units[i]
    for third in range(3):
        by_degree[128 * third : 128 * (third + 1)] = jnp.broadcast_to(summed[third : third + 1], (128, 128)).T
    first_degree = pl.multiple_of(b * DEGREES, DEGREES)
    degree = (first_degree + lax.broadcasted_iota(jnp.int32, (DEGREES, 128), 0)).astype(jnp.float32)
    spread = by_degree[pl.ds(first_degree, DEGREES)] / ((MEMBERS - 1) * CHANNELS * (2.0 * degree + 1.0))
    square = jnp.concatenate([spread, jnp.zeros((128 - DEGREES, 128), jnp.float32)], axis=0)
    spread_ref[...] = square.T[:8]
    scale = jnp.concatenate([lax.rsqrt(spread + EPSILON)] * 3, axis=1)
    for degree in range(DEGREES):
        out_ref[degree] = (turned[degree] * scale[degree : degree + 1]).astype(jnp.bfloat16)

    for chunk in range(2):
        wait_bytes(recv.at[chunk, pl.ds(0, LON - 1)], grid_send.at[chunk])
        wait_bytes(sent.at[chunk, pl.ds(0, UNITS * (LON - 1))], spec_send.at[chunk])

    @pl.when(has_piece(g, 2))
    def _():
        wait_bytes(recv.at[2, pl.ds(0, 25)], grid_send.at[2])
        wait_bytes(sent.at[2, pl.ds(0, UNITS * (LON - 1))], spec_send.at[2])

    @pl.when(jnp.logical_not(has_piece(g, 2)))
    def _():
        wait_bytes(recv.at[pl.ds(0, 2), pl.ds(0, 19), :, pl.ds(0, 256)], grid_send.at[2])
        wait_bytes(sent.at[2, pl.ds(0, UNITS * (LON - 1)), :, pl.ds(0, 256)], spec_send.at[2])

    for chunk in range(CHUNKS):
        wait_bytes(mixed.at[chunk, pl.ds(0, LAT - 1)], mix_send.at[chunk])
    wait_bytes(rest_in.at[pl.ds(0, LON - 1)], rest_send)
    wait_bytes(leg_raw.at[pl.ds(0, LAT - 1)], leg_send)
    wait_bytes(coeffs.at[pl.ds(0, LAT - 1)], coef_send)
    wait_bytes(all_squares.at[pl.ds(0, LON - 1)], sq_send)
    wait_bytes(all_units.at[pl.ds(0, LAT - 1)], unit_send)


def shards(grid, legendre):
    main, rest = [jnp.asarray(table) for table in spectral_table()]
    dma = pltpu.SemaphoreType.DMA
    bf16, f32 = jnp.bfloat16, jnp.float32
    any_space = pl.BlockSpec(memory_space=pl.ANY)
    vmem = pl.BlockSpec(memory_space=pltpu.VMEM)
    normalized, spread = pl.pallas_call(
        kernel,
        out_shape=(
            jax.ShapeDtypeStruct((DEGREES, 2 * ORDERS, FIELDS), bf16),
            jax.ShapeDtypeStruct((8, 128), f32),
        ),
        in_specs=[any_space] * 4,
        out_specs=(vmem, vmem),
        scratch_shapes=[
            pltpu.VMEM((CHUNKS, LON, MAIN, FIELDS), bf16),
            pltpu.VMEM((ROWS, REST, FIELDS), bf16),
            pltpu.VMEM((LON, REST_PAD, FIELDS), bf16),
            pltpu.VMEM((LON, REST_PAD, FIELDS), bf16),
            pltpu.VMEM((2 * DEG, LON * MAIN), bf16),
            pltpu.VMEM((CHUNKS, 2 * DEG, LON * REST_PAD), bf16),
            pltpu.VMEM((CHUNKS, LAT, LON * UNITS, FIELDS), bf16),
            pltpu.VMEM((CHUNKS, LAT, LON * UNITS, FIELDS), bf16),
            pltpu.VMEM((CHUNKS, LON * UNITS, LAT, FIELDS), bf16),
            pltpu.VMEM((UNITS, JPAD, LAT, FIELDS), bf16),
            pltpu.VMEM((LAT, 2, ROWS, DEG), bf16),
            pltpu.VMEM((2, DEG, JPAD * LAT), bf16),
            pltpu.VMEM((UNITS, DEG, FIELDS), f32),
            pltpu.VMEM((LAT, UNITS, DEGREES, FIELDS), bf16),
            pltpu.VMEM((LAT, UNITS, DEGREES, FIELDS), bf16),
            pltpu.VMEM((DEGREES, 2 * ORDERS, FIELDS), f32),
            pltpu.VMEM((DEG, 128), f32),
            pltpu.VMEM((3, 128), f32),
            pltpu.VMEM((LON, 3, 128), f32),
            pltpu.VMEM((3, 128), f32),
            pltpu.VMEM((LAT, 3, 128), f32),
            pltpu.VMEM((256, 256), bf16),
            pltpu.VMEM((128, 128), bf16),
            pltpu.VMEM((384, 384), bf16),
            dma((2,)),
            dma,
            dma((CHUNKS,)),
            dma((CHUNKS,)),
            dma,
            dma,
            dma,
            dma,
            dma((CHUNKS,)),
            dma((CHUNKS,)),
            dma((CHUNKS,)),
            dma,
            dma((UNITS,)),
            dma,
            dma,
            dma,
            dma,
            dma,
            dma,
        ],
        compiler_params=pltpu.CompilerParams(
            collective_id=0, has_side_effects=True, vmem_limit_bytes=48 * 1024 * 1024
        ),
        cost_estimate=pl.CostEstimate(flops=4_000_000_000, bytes_accessed=8_000_000, transcendentals=0),
    )(*[pltpu.with_memory_space_constraint(x, pltpu.HBM) for x in (grid, legendre, main, rest)])
    return normalized.reshape(DEGREES, ORDERS, 2, FIELDS), spread[0, :DEGREES]


def solution(mesh):
    return jax.shard_map(
        shards,
        mesh=mesh,
        in_specs=(P("lat", "lon", None), P("lon", "lat", None)),
        out_specs=(P("lat", "lon", None, None), P("lat")),
        check_vma=False,
    )
```

```python
import functools
import math

import jax
import jax.numpy as jnp
import numpy as np
from jax import lax
from jax.experimental import pallas as pl
from jax.experimental.pallas import tpu as pltpu
from jax.sharding import PartitionSpec as P

NLON = 1440
DEG = 384
CHANNELS = 64
MEMBERS = 6
FIELDS = 384
LAT = 8
LON = 32
ROWS = 90
LON_ROWS = 45
MAIN = 40
REST = LON_ROWS - MAIN
REST_PAD = 16
ORDERS = 12
DEGREES = 48
UNITS = 3
CHUNKS = 3
JPAD = 96
EPSILON = 1e-06
MESH = pl.DeviceIdType.MESH
GROUPS = ((0, 2), (2, 1))


def spectral_table():
    k = np.arange(NLON, dtype=np.int64)[:, None]
    m = np.arange(DEG, dtype=np.int64)[None, :]
    angle = ((k * m) % NLON).astype(np.float32) * np.float32(2.0 * math.pi / NLON)
    table = np.stack([np.cos(angle), -np.sin(angle)], axis=2).astype(np.float32)
    table = table.reshape(LON, LON_ROWS, LON, LAT, UNITS)
    table = table.transpose(3, 2, 4, 0, 1).reshape(2 * DEG, LON, LON_ROWS)
    rest = np.zeros((2 * DEG, LON, REST_PAD), np.float32)
    rest[:, :, :REST] = table[:, :, MAIN:]
    main = table[:, :, :MAIN].reshape(2 * DEG, LON * MAIN)
    return main.astype(jnp.bfloat16), rest.reshape(2 * DEG, LON * REST_PAD).astype(jnp.bfloat16)


def wait_bytes(ref, sem):
    pltpu.make_async_copy(ref, ref, sem).wait()


def swap_matrix(major, minor):
    size = major * minor
    out_row = lax.broadcasted_iota(jnp.int32, (size, size), 0)
    in_row = lax.broadcasted_iota(jnp.int32, (size, size), 1)
    wanted = (out_row % major) * minor + out_row // major
    return (in_row == wanted).astype(jnp.float32).astype(jnp.bfloat16)


def kernel(
    grid_ref,
    leg_ref,
    main_ref,
    rest_ref,
    out_ref,
    spread_ref,
    recv,
    rest_raw,
    rest_out,
    rest_in,
    basis,
    rest_basis,
    spec,
    mixed,
    sent,
    spectral,
    leg_raw,
    leg,
    begun,
    part,
    coeffs,
    turned,
    by_degree,
    squares,
    all_squares,
    unit_squares,
    all_units,
    swap_spec,
    swap_leg,
    swap_out,
    basis_sem,
    raw_sem,
    grid_send,
    grid_recv,
    rest_send,
    rest_recv,
    leg_send,
    leg_recv,
    mix_send,
    mix_recv,
    spec_send,
    spec_recv,
    last_recv,
    coef_send,
    coef_recv,
    sq_send,
    sq_recv,
    unit_send,
    unit_recv,
):
    b = lax.axis_index("lat")
    g = lax.axis_index("lon")

    def lon_peer(i):
        return (g + i) % LON

    def lat_peer(i):
        return (b + i) % LAT

    def first_piece(d):
        return 39 * d // 16

    def has_piece(d, k):
        return first_piece(d) + k < first_piece(d + 1)

    def piece_of(d, k):
        piece = first_piece(d) + k
        return 2 * LON + piece // 3, pl.ds(pl.multiple_of(128 * (piece % 3), 128), 128)

    def each_piece(d, action):
        for k in range(CHUNKS):
            row, fields = piece_of(d, k)
            run = functools.partial(action, row, fields, pl.ds(128 * k, 128))
            if k < 2:
                run()
            else:
                pl.when(has_piece(d, k))(run)

    def to_lon(src, dst, send_sem, recv_sem, d):
        pltpu.make_async_remote_copy(
            src_ref=src, dst_ref=dst, send_sem=send_sem, recv_sem=recv_sem, device_id={"lon": d}, device_id_type=MESH
        ).start()

    def to_lat(src, dst, send_sem, recv_sem, d):
        pltpu.make_async_remote_copy(
            src_ref=src, dst_ref=dst, send_sem=send_sem, recv_sem=recv_sem, device_id={"lat": d}, device_id_type=MESH
        ).start()

    raw_copy = pltpu.make_async_copy(grid_ref.at[:, pl.ds(MAIN, REST)], rest_raw, raw_sem)
    raw_copy.start()
    basis_copy = pltpu.make_async_copy(main_ref, basis, basis_sem.at[0])
    basis_copy.start()
    first_rest_copy = pltpu.make_async_copy(rest_ref, rest_basis.at[0], basis_sem.at[1])
    first_rest_copy.start()
    barrier = pltpu.get_barrier_semaphore()

    @pl.loop(1, LON)
    def _(i):
        pl.semaphore_signal(barrier, inc=1, device_id={"lon": lon_peer(i)}, device_id_type=MESH)

    @pl.loop(1, LAT)
    def _(i):
        pl.semaphore_signal(barrier, inc=1, device_id={"lat": lat_peer(i)}, device_id_type=MESH)

    pl.semaphore_wait(barrier, LON + LAT - 2)

    def send_rows(chunk):
        @pl.loop(1, LON)
        def _(i):
            d = lon_peer(i)
            src = grid_ref.at[chunk * LON + d, pl.ds(0, MAIN)]
            to_lon(src, recv.at[chunk, g], grid_send.at[chunk], grid_recv.at[chunk], d)

        src = grid_ref.at[chunk * LON + g, pl.ds(0, MAIN)]
        pltpu.make_async_copy(src, recv.at[chunk, g], grid_recv.at[chunk]).start()

    send_rows(0)

    @pl.loop(1, LAT)
    def _(i):
        u = lat_peer(i)
        to_lat(leg_ref.at[pl.ds(UNITS * u // 2, 2)], leg_raw.at[b], leg_send, leg_recv, u)

    pltpu.make_async_copy(leg_ref.at[pl.ds(UNITS * b // 2, 2)], leg_raw.at[b], leg_recv).start()

    raw_copy.wait()

    @pl.loop(0, LON)
    def _(d):
        pieces = [rest_raw[d].astype(jnp.float32), rest_raw[LON + d].astype(jnp.float32)]
        last = []
        for k in range(CHUNKS):
            row, fields = piece_of(d, k)
            last.append(rest_raw[row, :, fields].astype(jnp.float32))
        last[2] = jnp.where(has_piece(d, 2), last[2], 0.0)
        pieces += [jnp.concatenate(last, axis=1), jnp.zeros((1, FIELDS), jnp.float32)]
        rest_out[d] = jnp.concatenate(pieces, axis=0).astype(jnp.bfloat16)

    @pl.loop(1, LON)
    def _(i):
        d = lon_peer(i)
        to_lon(rest_out.at[d], rest_in.at[g], rest_send, rest_recv, d)

    pltpu.make_async_copy(rest_out.at[g], rest_in.at[g], rest_recv).start()
    send_rows(1)

    @pl.loop(1, LON)
    def _(i):
        d = lon_peer(i)

        def send(row, fields, lanes):
            src = grid_ref.at[row, pl.ds(0, MAIN), fields]
            to_lon(src, recv.at[2, g, :, lanes], grid_send.at[2], grid_recv.at[2], d)

        each_piece(d, send)

    def keep(row, fields, lanes):
        src = grid_ref.at[row, pl.ds(0, MAIN), fields]
        pltpu.make_async_copy(src, recv.at[2, g, :, lanes], grid_recv.at[2]).start()

    each_piece(g, keep)

    @pl.when(jnp.logical_not(has_piece(g, 2)))
    def _():
        recv[2, :, :, 256:] = jnp.zeros((LON, MAIN, 128), recv.dtype)

    swap_spec[...] = swap_matrix(LAT, 32)
    swap_leg[...] = swap_matrix(LAT, 16)
    swap_out[...] = swap_matrix(2 * ORDERS, 16)
    spectral[:, ROWS:] = jnp.zeros((UNITS, JPAD - ROWS, LAT, FIELDS), spectral.dtype)

    first_rest_copy.wait()
    size = LON * REST_PAD
    from_column = lax.broadcasted_iota(jnp.int32, (size, size), 0)
    to_column = lax.broadcasted_iota(jnp.int32, (size, size), 1)
    for chunk in range(1, CHUNKS):
        move = (from_column + REST * chunk == to_column).astype(jnp.float32).astype(jnp.bfloat16)
        moved = jnp.dot(rest_basis[0], move, preferred_element_type=jnp.float32)
        rest_basis[chunk] = moved.astype(jnp.bfloat16)

    wait_bytes(leg_raw, leg_recv)
    for which in range(2):
        for block in range(JPAD // 16):
            first = 16 * block
            rows = min(16, ROWS - first)
            piece = leg_raw[:, which, first : first + rows, :].astype(jnp.float32)
            if rows < 16:
                piece = jnp.concatenate([piece, jnp.zeros((LAT, 16 - rows, DEG), jnp.float32)], axis=1)
            piece = piece.reshape(LAT * 16, DEG).astype(jnp.bfloat16)
            moved = jnp.dot(swap_leg[...], piece, preferred_element_type=jnp.float32)
            leg[which, :, 128 * block : 128 * (block + 1)] = moved.T.astype(jnp.bfloat16)

    def send_spectrum(chunk):
        row = chunk * LON + g

        @pl.loop(1, LON)
        def _(i):
            d = lon_peer(i)
            src = sent.at[chunk, pl.ds(UNITS * d, UNITS)]
            to_lon(src, spectral.at[:, row], spec_send.at[chunk], spec_recv, d)

        pltpu.make_async_copy(sent.at[chunk, pl.ds(UNITS * g, UNITS)], spectral.at[:, row], spec_recv).start()

    def send_last():
        for part_id, (first, count) in enumerate(GROUPS):

            @pl.loop(1, LON)
            def _(i):
                d = lon_peer(i)

                def send(row, fields, lanes):
                    src = sent.at[2, pl.ds(UNITS * d + first, count), :, lanes]
                    dst = spectral.at[pl.ds(first, count), row, :, fields]
                    to_lon(src, dst, spec_send.at[2], last_recv.at[part_id], d)

                each_piece(g, send)

            def keep(row, fields, lanes):
                src = sent.at[2, pl.ds(UNITS * g + first, count), :, lanes]
                dst = spectral.at[pl.ds(first, count), row, :, fields]
                pltpu.make_async_copy(src, dst, last_recv.at[part_id]).start()

            each_piece(g, keep)

    basis_copy.wait()
    wait_bytes(rest_in, rest_recv)

    @pl.loop(0, CHUNKS)
    def _(chunk):
        @pl.when((chunk < 2) | has_piece(g, 2))
        def _():
            wait_bytes(recv.at[chunk], grid_recv.at[chunk])

        @pl.when((chunk == 2) & jnp.logical_not(has_piece(g, 2)))
        def _():
            wait_bytes(recv.at[chunk, :, :, pl.ds(0, 256)], grid_recv.at[chunk])

        values = recv[chunk].astype(jnp.float32).reshape(LON * MAIN, FIELDS).astype(jnp.bfloat16)
        rows = jnp.dot(basis[...], values, preferred_element_type=jnp.float32)
        values = rest_in[...].reshape(LON * REST_PAD, FIELDS)
        rows = rows + jnp.dot(rest_basis[chunk], values, preferred_element_type=jnp.float32)
        spec[chunk] = rows.astype(jnp.bfloat16).reshape(LAT, LON * UNITS, FIELDS)

        @pl.loop(1, LAT)
        def _(i):
            u = lat_peer(i)
            to_lat(spec.at[chunk, u], mixed.at[chunk, b], mix_send.at[chunk], mix_recv.at[chunk], u)

        pltpu.make_async_copy(spec.at[chunk, b], mixed.at[chunk, b], mix_recv.at[chunk]).start()
        wait_bytes(mixed.at[chunk], mix_recv.at[chunk])
        for block in range(3):
            piece = mixed[chunk, :, 32 * block : 32 * (block + 1), :].reshape(LAT * 32, FIELDS)
            moved = jnp.dot(swap_spec[...], piece, preferred_element_type=jnp.float32)
            sent[chunk, 32 * block : 32 * (block + 1)] = moved.reshape(32, LAT, FIELDS).astype(jnp.bfloat16)
        pl.when(chunk < 2)(lambda: send_spectrum(chunk))
        pl.when(chunk == 2)(send_last)

    early = 2 * LON
    wait_bytes(spectral.at[:, pl.ds(0, early)], spec_recv)

    def table_of(unit):
        return (UNITS * b + unit) // 2 - UNITS * b // 2

    for unit in range(UNITS):
        values = spectral[unit, :early].astype(jnp.float32).reshape(early * LAT, FIELDS).astype(jnp.bfloat16)
        begun[unit] = jnp.dot(leg[table_of(unit), :, : early * LAT], values, preferred_element_type=jnp.float32)
    for unit in range(UNITS):
        for part_id, (first, count) in enumerate(GROUPS):
            if first == unit:
                wait_bytes(spectral.at[pl.ds(first, count), pl.ds(early, ROWS - early)], last_recv.at[part_id])
        values = spectral[unit, early:].astype(jnp.float32).reshape((JPAD - early) * LAT, FIELDS).astype(jnp.bfloat16)
        total = jnp.dot(leg[table_of(unit), :, early * LAT :], values, preferred_element_type=jnp.float32)
        total = begun[unit] + total
        part[:, unit] = total.astype(jnp.bfloat16).reshape(LAT, DEGREES, FIELDS)

        @pl.loop(1, LAT)
        def _(i):
            u = lat_peer(i)
            to_lat(part.at[u, unit], coeffs.at[b, unit], coef_send, coef_recv, u)

        pltpu.make_async_copy(part.at[b, unit], coeffs.at[b, unit], coef_recv).start()
        tiles = [total[:, 128 * t : 128 * (t + 1)] for t in range(3)]
        both = tiles[0] + tiles[1] + tiles[2]
        mean = (both + pltpu.roll(both, CHANNELS, 1)) * (1.0 / MEMBERS)
        square = sum((tile - mean) * (tile - mean) for tile in tiles)
        by_degree[...] = square if unit == 0 else by_degree[...] + square

    for third in range(3):
        rows = by_degree[128 * third : 128 * (third + 1)]
        squares[third : third + 1] = jnp.sum(rows.T, axis=0, keepdims=True)

    @pl.loop(1, LON)
    def _(i):
        to_lon(squares, all_squares.at[g], sq_send, sq_recv, lon_peer(i))

    pltpu.make_async_copy(squares, all_squares.at[g], sq_recv).start()
    wait_bytes(all_squares, sq_recv)
    summed = all_squares[0]
    for i in range(1, LON):
        summed = summed + all_squares[i]
    unit_squares[...] = summed

    @pl.loop(1, LAT)
    def _(i):
        to_lat(unit_squares, all_units.at[b], unit_send, unit_recv, lat_peer(i))

    pltpu.make_async_copy(unit_squares, all_units.at[b], unit_recv).start()
    wait_bytes(coeffs, coef_recv)
    for block in range(3):
        x = coeffs[:, :, 16 * block : 16 * (block + 1), :].reshape(2 * ORDERS * 16, FIELDS)
        moved = jnp.dot(swap_out[...], x, preferred_element_type=jnp.float32)
        turned[16 * block : 16 * (block + 1)] = moved.reshape(16, 2 * ORDERS, FIELDS)

    wait_bytes(all_units, unit_recv)
    summed = all_units[0]
    for i in range(1, LAT):
        summed = summed + all_units[i]
    for third in range(3):
        by_degree[128 * third : 128 * (third + 1)] = jnp.broadcast_to(summed[third : third + 1], (128, 128)).T
    first_degree = pl.multiple_of(b * DEGREES, DEGREES)
    degree = (first_degree + lax.broadcasted_iota(jnp.int32, (DEGREES, 128), 0)).astype(jnp.float32)
    spread = by_degree[pl.ds(first_degree, DEGREES)] / ((MEMBERS - 1) * CHANNELS * (2.0 * degree + 1.0))
    square = jnp.concatenate([spread, jnp.zeros((128 - DEGREES, 128), jnp.float32)], axis=0)
    spread_ref[...] = square.T[:8]
    scale = jnp.concatenate([lax.rsqrt(spread + EPSILON)] * 3, axis=1)
    for degree in range(DEGREES):
        out_ref[degree] = (turned[degree] * scale[degree : degree + 1]).astype(jnp.bfloat16)

    for chunk in range(2):
        wait_bytes(recv.at[chunk, pl.ds(0, LON - 1)], grid_send.at[chunk])
        wait_bytes(sent.at[chunk, pl.ds(0, UNITS * (LON - 1))], spec_send.at[chunk])

    @pl.when(has_piece(g, 2))
    def _():
        wait_bytes(recv.at[2, pl.ds(0, 25)], grid_send.at[2])
        wait_bytes(sent.at[2, pl.ds(0, UNITS * (LON - 1))], spec_send.at[2])

    @pl.when(jnp.logical_not(has_piece(g, 2)))
    def _():
        wait_bytes(recv.at[pl.ds(0, 2), pl.ds(0, 19), :, pl.ds(0, 256)], grid_send.at[2])
        wait_bytes(sent.at[2, pl.ds(0, UNITS * (LON - 1)), :, pl.ds(0, 256)], spec_send.at[2])

    for chunk in range(CHUNKS):
        wait_bytes(mixed.at[chunk, pl.ds(0, LAT - 1)], mix_send.at[chunk])
    wait_bytes(rest_in.at[pl.ds(0, LON - 1)], rest_send)
    wait_bytes(leg_raw.at[pl.ds(0, LAT - 1)], leg_send)
    wait_bytes(coeffs.at[pl.ds(0, LAT - 1)], coef_send)
    wait_bytes(all_squares.at[pl.ds(0, LON - 1)], sq_send)
    wait_bytes(all_units.at[pl.ds(0, LAT - 1)], unit_send)


def shards(grid, legendre):
    main, rest = [jnp.asarray(table) for table in spectral_table()]
    dma = pltpu.SemaphoreType.DMA
    bf16, f32 = jnp.bfloat16, jnp.float32
    any_space = pl.BlockSpec(memory_space=pl.ANY)
    vmem = pl.BlockSpec(memory_space=pltpu.VMEM)
    normalized, spread = pl.pallas_call(
        kernel,
        out_shape=(
            jax.ShapeDtypeStruct((DEGREES, 2 * ORDERS, FIELDS), bf16),
            jax.ShapeDtypeStruct((8, 128), f32),
        ),
        in_specs=[any_space] * 4,
        out_specs=(vmem, vmem),
        scratch_shapes=[
            pltpu.VMEM((CHUNKS, LON, MAIN, FIELDS), bf16),
            pltpu.VMEM((ROWS, REST, FIELDS), bf16),
            pltpu.VMEM((LON, REST_PAD, FIELDS), bf16),
            pltpu.VMEM((LON, REST_PAD, FIELDS), bf16),
            pltpu.VMEM((2 * DEG, LON * MAIN), bf16),
            pltpu.VMEM((CHUNKS, 2 * DEG, LON * REST_PAD), bf16),
            pltpu.VMEM((CHUNKS, LAT, LON * UNITS, FIELDS), bf16),
            pltpu.VMEM((CHUNKS, LAT, LON * UNITS, FIELDS), bf16),
            pltpu.VMEM((CHUNKS, LON * UNITS, LAT, FIELDS), bf16),
            pltpu.VMEM((UNITS, JPAD, LAT, FIELDS), bf16),
            pltpu.VMEM((LAT, 2, ROWS, DEG), bf16),
            pltpu.VMEM((2, DEG, JPAD * LAT), bf16),
            pltpu.VMEM((UNITS, DEG, FIELDS), f32),
            pltpu.VMEM((LAT, UNITS, DEGREES, FIELDS), bf16),
            pltpu.VMEM((LAT, UNITS, DEGREES, FIELDS), bf16),
            pltpu.VMEM((DEGREES, 2 * ORDERS, FIELDS), f32),
            pltpu.VMEM((DEG, 128), f32),
            pltpu.VMEM((3, 128), f32),
            pltpu.VMEM((LON, 3, 128), f32),
            pltpu.VMEM((3, 128), f32),
            pltpu.VMEM((LAT, 3, 128), f32),
            pltpu.VMEM((256, 256), bf16),
            pltpu.VMEM((128, 128), bf16),
            pltpu.VMEM((384, 384), bf16),
            dma((2,)),
            dma,
            dma((CHUNKS,)),
            dma((CHUNKS,)),
            dma,
            dma,
            dma,
            dma,
            dma((CHUNKS,)),
            dma((CHUNKS,)),
            dma((CHUNKS,)),
            dma,
            dma((UNITS,)),
            dma,
            dma,
            dma,
            dma,
            dma,
            dma,
        ],
        compiler_params=pltpu.CompilerParams(
            collective_id=0, has_side_effects=True, vmem_limit_bytes=48 * 1024 * 1024
        ),
        cost_estimate=pl.CostEstimate(flops=4_000_000_000, bytes_accessed=8_000_000, transcendentals=0),
    )(*[pltpu.with_memory_space_constraint(x, pltpu.HBM) for x in (grid, legendre, main, rest)])
    return normalized.reshape(DEGREES, ORDERS, 2, FIELDS), spread[0, :DEGREES]


def solution(mesh):
    return jax.shard_map(
        shards,
        mesh=mesh,
        in_specs=(P("lat", "lon", None), P("lon", "lat", None)),
        out_specs=(P("lat", "lon", None, None), P("lat")),
        check_vma=False,
    )
```
